32 devices in a mesh: leaf: 8 (over y, x, core), sub: 4 (over z).
Axes of the slice: x: 2, y: 2, z: 4, core: 2. Of those that a mesh axis runs over, the one named last changes fastest.
Arguments:
- currents: float32 [65536, 128], P(('leaf', 'sub')), may hold values from -6 to 6
- leaf_basis: float32 [512, 128, 128], P(('leaf', 'sub')), may hold values from -0.5 to 0.5
- leaf_rank: int32 [512], P(('leaf', 'sub')), may hold values from 64 to 128
- leaf_transfer: float32 [512, 128, 128], P(('leaf', 'sub')), may hold values from -0.25 to 0.25
- top_transfer: float32 [8, 4, 128, 128], P('leaf', None, None, 'sub'), may hold values from -0.375 to 0.375
- far_table: float32 [32, 2, 128, 128], replicated, may hold values from -0.125 to 0.125
- send_src: int32 [32, 3, 4, 12], P(('leaf', 'sub')), may hold values from -1 to 15, as said below
- recv_tgt: int32 [32, 3, 4, 12], P(('leaf', 'sub')), may hold values from -1 to 15, as said below
- recv_type: int32 [32, 3, 4, 12], P(('leaf', 'sub')), may hold values from 0 to 31, as said below
- top_coupling: float32 [8, 4, 2, 128, 128], P('leaf', None, None, 'sub'), may hold values from -0.1875 to 0.1875
- top_list: int32 [8, 4], P('leaf'), may hold values from 0 to 7, as said below
- near_blocks: float32 [2048, 2, 128, 128], P(('leaf', 'sub')), may hold values from -0.1875 to 0.1875
- near_tgt: int32 [32, 64], P(('leaf', 'sub')), may hold values from 0 to 15, as said below
- near_src: int32 [32, 64], P(('leaf', 'sub')), may hold values from 0 to 23, as said below
Outputs:
- potential: float32 [65536, 128], P(('leaf', 'sub'))
The draws below stay inside these ranges and needn't reach their ends.
Inputs may be any that keep to these rules, and one draw needn't show every extreme that they name: `send_src`: entry [q, o, s, j] names the leaf of device q (counted from its first leaf) whose coefficients fill slot j of what device q sends to device (q // 4 + o - 1) * 4 + s, or -1 for an empty slot; it is -1 wherever q // 4 + o - 1 lies outside 0 to 7. In every draw some device receives 12 filled slots from every device of its own group and of the two groups beside it. `recv_tgt`: entry [p, o, s, j] is the leaf of device p (counted from its first leaf) on which slot j from device (p // 4 + o - 1) * 4 + s acts; it is -1 exactly where that slot is empty or that device does not exist. `recv_type`: entry [p, o, s, j] selects the matrix of far_table for slot j from device (p // 4 + o - 1) * 4 + s to device p. `top_list`: row g names 4 different groups, none equal to g. `near_tgt`: counted from the device's first leaf. `near_src`: counted from 4 leaves before the device's first leaf; it lies within 4 leaves of the block's target leaf.
All inputs are finite; a program needn't handle non-finite values.
Results may differ from the reference program's by a relative error of at most 0.0003.
Values sent between devices are 32-bit elements; how exact they have to be, the bound alone decides.
A program may use at most 192 MiB of HBM per device.

```python
import jax
import jax.numpy as jnp
from jax import lax

PANEL = 128
RANK = 128
LEAF_DEV = 16
CAP = 12
NEAR_DEV = 64
HALO_L = 4
NTYPE = 32
K_TOP = 4
DEVS = 32
GROUPS = 8
NLEAVES = 512
PANELS = 65536
COLS = 128
N_SUB = 4


def far_plan(key):
    base = jax.random.fold_in(key, 17)
    fill_key, roll_key, full_key, source_key, target_key, kind_key = jax.random.split(base, 6)
    fill_share = jax.random.randint(fill_key, (DEVS,), 25, 76)
    roll_value = jax.random.randint(roll_key, (DEVS, 3, N_SUB, CAP), 0, 100)
    full_dest = jax.random.randint(full_key, (), N_SUB, DEVS - N_SUB)
    sender_ids = jnp.arange(DEVS, dtype=jnp.int32)[:, None, None, None]
    offsets = jnp.arange(3, dtype=jnp.int32)[None, :, None, None]
    subs = jnp.arange(N_SUB, dtype=jnp.int32)[None, None, :, None]
    receiver_group = sender_ids // N_SUB + offsets - 1
    receiver_valid = (receiver_group >= 0) & (receiver_group < GROUPS)
    receiver = jnp.clip(receiver_group, 0, GROUPS - 1) * N_SUB + subs
    used_slot = ((roll_value < fill_share[receiver]) | (receiver == full_dest)) & receiver_valid
    source_leaf = jax.random.randint(source_key, (DEVS, 3, N_SUB, CAP), 0, LEAF_DEV)
    target_leaf = jax.random.randint(target_key, (DEVS, 3, N_SUB, CAP), 0, LEAF_DEV)
    kind_ids = jax.random.randint(kind_key, (DEVS, 3, N_SUB, CAP), 0, NTYPE)
    return (used_slot, source_leaf, target_leaf, kind_ids)


def receiver_view(values):
    receivers = jnp.arange(DEVS, dtype=jnp.int32)
    group = receivers // N_SUB
    sub_index = receivers % N_SUB
    offsets = jnp.arange(3, dtype=jnp.int32)
    sender_groups = group[:, None] + offsets[None, :] - 1
    valid = (sender_groups >= 0) & (sender_groups < GROUPS)
    senders = jnp.clip(sender_groups, 0, GROUPS - 1)[:, :, None] * N_SUB + jnp.arange(N_SUB, dtype=jnp.int32)[None, None, :]
    back = jnp.broadcast_to((2 - offsets)[None, :, None], (DEVS, 3, N_SUB))
    subs = jnp.broadcast_to(sub_index[:, None, None], (DEVS, 3, N_SUB))
    return (values[senders, back, subs], jnp.broadcast_to(valid[:, :, None, None], (DEVS, 3, N_SUB, CAP)))


def draw_send_src(key, part):
    used_slot, source_leaf, target_leaf, kind_ids = far_plan(key)
    return jnp.where(used_slot, source_leaf, -1).astype(jnp.int32)


def draw_recv_tgt(key, part):
    used_slot, source_leaf, target_leaf, kind_ids = far_plan(key)
    used_view, valid = receiver_view(used_slot)
    target_view, valid = receiver_view(target_leaf)
    return jnp.where(used_view & valid, target_view, -1).astype(jnp.int32)


def draw_recv_type(key, part):
    used_slot, source_leaf, target_leaf, kind_ids = far_plan(key)
    kind_view, valid = receiver_view(kind_ids)
    return kind_view.astype(jnp.int32)


def near_plan(key):
    base = jax.random.fold_in(key, 29)
    target_key, offset_key = jax.random.split(base, 2)
    target_leaf = jax.random.randint(target_key, (DEVS, NEAR_DEV), 0, LEAF_DEV)
    offsets = jax.random.randint(offset_key, (DEVS, NEAR_DEV), -HALO_L, HALO_L + 1)
    return (target_leaf, target_leaf + HALO_L + offsets)


def draw_near_tgt(key, part):
    target_leaf, source_leaf = near_plan(key)
    return target_leaf.astype(jnp.int32)


def draw_near_src(key, part):
    target_leaf, source_leaf = near_plan(key)
    return source_leaf.astype(jnp.int32)


def draw_top_list(key, part):
    base = jax.random.fold_in(key, 41)
    scores = jax.random.randint(base, (GROUPS, GROUPS), 0, 4096) * GROUPS + jnp.arange(GROUPS, dtype=jnp.int32)[None, :]
    diagonal = jnp.arange(GROUPS, dtype=jnp.int32)[:, None] == jnp.arange(GROUPS, dtype=jnp.int32)[None, :]
    scores = jnp.where(diagonal, 2 ** 30, scores)
    ordering = jnp.argsort(scores, axis=1)
    return ordering[:, :K_TOP].astype(jnp.int32)


def place_ends(array, key, smallest, largest):
    longest = array.shape.index(max(array.shape))
    spots = []
    for shift in (0, 1):
        where = [jax.random.randint(jax.random.fold_in(key, axis), (), 0, length) for axis, length in enumerate(array.shape)]
        where[longest] = (where[longest] + shift) % array.shape[longest]
        spots.append(tuple(where))
    return array.at[spots[0]].set(smallest).at[spots[1]].set(largest)


def shard_levels(stream_key, extent, cuts, smallest, top_value):
    level, own = 1.0, jax.random.fold_in(stream_key, 6)
    for axis_at, parts in cuts:
        steps = jnp.exp(jax.random.uniform(jax.random.fold_in(own, axis_at), (parts,), jnp.float32, smallest / len(cuts), top_value / len(cuts)))
        level = level * jnp.repeat(steps, extent[axis_at] // parts).reshape([-1 if axis == axis_at else 1 for axis in range(len(extent))])
    return level


def scatter_about(own_key, extent, scale, bound, shards=(), kind=jnp.bfloat16):
    factor_of = shard_levels(own_key, extent, shards, -0.22, 0.18) if shards else 1.0
    entries = jax.random.normal(own_key, extent, jnp.float32) * scale * factor_of
    return jnp.minimum(jnp.maximum(entries, -bound), bound).astype(kind)


def setup_inputs(seed: int = 0) -> dict:
    key_of = jax.random.split(jax.random.key(seed), 15)
    return {
        "currents": scatter_about(key_of[0], (PANELS, COLS), 1.0, 6.0, ((0, 32),), jnp.float32),
        "leaf_basis": scatter_about(key_of[1], (NLEAVES, PANEL, RANK), PANEL ** -0.5, 0.5, ((0, 32),), jnp.float32),
        "leaf_rank": place_ends(jax.random.randint(key_of[2], (NLEAVES,), RANK // 2, RANK + 1), jax.random.fold_in(key_of[2], 1), RANK // 2, RANK).astype(jnp.int32),
        "leaf_transfer": scatter_about(key_of[3], (NLEAVES, RANK, RANK), (4 * RANK) ** -0.5, 0.25, ((0, 32),), jnp.float32),
        "top_transfer": scatter_about(key_of[4], (GROUPS, N_SUB, RANK, RANK), (2 * RANK) ** -0.5, 0.375, ((0, 8), (3, 4)), jnp.float32),
        "far_table": scatter_about(key_of[5], (NTYPE, 2, RANK, RANK), (2 * RANK * 3 * N_SUB * CAP // LEAF_DEV) ** -0.5, 0.125, (), jnp.float32),
        "send_src": draw_send_src(jax.random.fold_in(key_of[14], 71), 0),
        "recv_tgt": draw_recv_tgt(jax.random.fold_in(key_of[14], 71), 0),
        "recv_type": draw_recv_type(jax.random.fold_in(key_of[14], 71), 0),
        "top_coupling": scatter_about(key_of[9], (GROUPS, K_TOP, 2, RANK, RANK), (2 * RANK * K_TOP) ** -0.5, 0.1875, ((0, 8), (3, 4)), jnp.float32),
        "top_list": draw_top_list(jax.random.fold_in(key_of[14], 71), 0),
        "near_blocks": scatter_about(key_of[11], (DEVS * NEAR_DEV, 2, PANEL, PANEL), (2 * PANEL * NEAR_DEV // LEAF_DEV) ** -0.5, 0.1875, ((0, 32),), jnp.float32),
        "near_tgt": draw_near_tgt(jax.random.fold_in(key_of[14], 71), 0),
        "near_src": draw_near_src(jax.random.fold_in(key_of[14], 71), 0),
    }


exact_precision = lax.Precision.HIGHEST


def rotate(values):
    middle = values.shape[-1] // 2
    return jnp.concatenate([-values[..., middle:], values[..., :middle]], axis=-1)


def far_device(device, leaf_coef, send_src, recv_tgt, recv_type, far_table):
    group = device // N_SUB
    sub_index = device % N_SUB
    offsets = jnp.arange(3, dtype=jnp.int32)
    sender_groups = group + offsets - 1
    valid = (sender_groups >= 0) & (sender_groups < GROUPS)
    senders = jnp.clip(sender_groups, 0, GROUPS - 1)[:, None] * N_SUB + jnp.arange(N_SUB, dtype=jnp.int32)[None, :]
    back = jnp.broadcast_to((2 - offsets)[:, None], (3, N_SUB))
    sources = send_src[senders, back, sub_index]
    sources = jnp.where(valid[:, None, None], sources, -1)
    leaf_ids = senders[:, :, None] * LEAF_DEV + jnp.maximum(sources, 0)
    present = (sources >= 0).astype(jnp.float32)
    gathered = leaf_coef[leaf_ids] * present[:, :, :, None, None]
    slot_count = 3 * N_SUB * CAP
    gathered = gathered.reshape(slot_count, RANK, gathered.shape[-1])
    kind_ids = lax.dynamic_index_in_dim(recv_type, device, axis=0, keepdims=False).reshape(slot_count)
    targets = lax.dynamic_index_in_dim(recv_tgt, device, axis=0, keepdims=False).reshape(slot_count)
    matrices = far_table[kind_ids]
    operator_product = jnp.einsum("sab,sbc->sac", matrices[:, 0], gathered, precision=exact_precision)
    operator_product = operator_product + jnp.einsum("sab,sbc->sac", matrices[:, 1], rotate(gathered), precision=exact_precision)
    selector_matrix = (targets[:, None] == jnp.arange(LEAF_DEV, dtype=jnp.int32)[None, :]).astype(jnp.float32)
    return jnp.einsum("iv,ibg->vbg", selector_matrix, operator_product, precision=exact_precision)


def near_device(device, leaf_currents, blocks, near_tgt, near_src):
    extended = lax.dynamic_index_in_dim(near_src, device, axis=0, keepdims=False)
    leaf_ids = device * LEAF_DEV + extended - HALO_L
    inside_grid = ((leaf_ids >= 0) & (leaf_ids < NLEAVES)).astype(jnp.float32)
    sources = leaf_currents[jnp.clip(leaf_ids, 0, NLEAVES - 1)] * inside_grid[:, None, None]
    own_blocks = lax.dynamic_index_in_dim(blocks, device, axis=0, keepdims=False)
    operator_product = jnp.einsum("nab,nbc->nac", own_blocks[:, 0], sources, precision=exact_precision)
    operator_product = operator_product + jnp.einsum("nab,nbc->nac", own_blocks[:, 1], rotate(sources), precision=exact_precision)
    targets = lax.dynamic_index_in_dim(near_tgt, device, axis=0, keepdims=False)
    selector_matrix = (targets[:, None] == jnp.arange(LEAF_DEV, dtype=jnp.int32)[None, :]).astype(jnp.float32)
    return jnp.einsum("if,ivo->fvo", selector_matrix, operator_product, precision=exact_precision)


def reference(currents, leaf_basis, leaf_rank, leaf_transfer, top_transfer, far_table, send_src, recv_tgt, recv_type, top_coupling, top_list, near_blocks, near_tgt, near_src):
    columns = currents.shape[1]
    rank_mask = (jnp.arange(RANK, dtype=jnp.int32)[None, :] < leaf_rank[:, None]).astype(jnp.float32)
    masked_basis = leaf_basis * rank_mask[:, None, :]
    leaf_currents = currents.reshape(NLEAVES, PANEL, columns)
    leaf_coef = jnp.einsum("lpr,lpc->lrc", masked_basis, leaf_currents, precision=exact_precision)
    lifted = jnp.einsum("lab,lac->lbc", leaf_transfer, leaf_coef, precision=exact_precision)
    mid_coef = lifted.reshape(DEVS, LEAF_DEV, RANK, columns).sum(axis=1)
    grouped = mid_coef.reshape(GROUPS, N_SUB, RANK, columns)
    top_coef = jnp.einsum("gsab,gsac->gbc", top_transfer, grouped, precision=exact_precision)
    partners = top_coef[top_list]
    top_field = jnp.einsum("gkab,gkbc->gac", top_coupling[:, :, 0], partners, precision=exact_precision)
    top_field = top_field + jnp.einsum("gkab,gkbc->gac", top_coupling[:, :, 1], rotate(partners), precision=exact_precision)
    mid_field = jnp.einsum("gsab,gbc->gsac", top_transfer, top_field, precision=exact_precision).reshape(DEVS, RANK, columns)
    down_field = jnp.einsum("lab,lbc->lac", leaf_transfer, jnp.repeat(mid_field, LEAF_DEV, axis=0), precision=exact_precision)
    far_field = lax.map(lambda device: far_device(device, leaf_coef, send_src, recv_tgt, recv_type, far_table), jnp.arange(DEVS, dtype=jnp.int32))
    leaf_field = far_field.reshape(NLEAVES, RANK, columns) + down_field
    far_part = jnp.einsum("lpr,lrc->lpc", masked_basis, leaf_field, precision=exact_precision)
    blocks = near_blocks.reshape(DEVS, NEAR_DEV, 2, PANEL, PANEL)
    near_field_share = lax.map(lambda device: near_device(device, leaf_currents, blocks, near_tgt, near_src), jnp.arange(DEVS, dtype=jnp.int32))
    near_field_share = near_field_share.reshape(NLEAVES, PANEL, columns)
    return (far_part + near_field_share).reshape(PANELS, columns)
```

```python
import functools

import jax
import jax.numpy as jnp
from jax import lax
from jax.experimental import pallas as pl
from jax.experimental.pallas import tpu as pltpu
from jax.sharding import PartitionSpec as P

HALO_L = 4
F32 = jnp.float32
BF16 = jnp.bfloat16
NN = (((1,), (0,)), ((), ()))
TN = (((0,), (0,)), ((), ()))


SMEM = pl.BlockSpec(memory_space=pltpu.SMEM)
VMEM = pl.BlockSpec(memory_space=pltpu.VMEM)


def shifted(value, axis, by):
    length = lax.axis_size(axis)
    pairs = [(i, i + by) for i in range(length) if 0 <= i + by < length]
    return lax.ppermute(value, axis, pairs)


def turned(value, by):
    length = lax.axis_size("sub")
    return lax.ppermute(value, "sub", [(i, (i + by) % length) for i in range(length)])


def gather_sub(value):
    return [value] + [turned(value, d) for d in range(1, lax.axis_size("sub"))]


def split(x):
    high = x.astype(BF16)
    return high, (x - high.astype(F32)).astype(BF16)


def dot(a, b, dims=NN):
    return lax.dot_general(a, b, dims, preferred_element_type=F32)


def dot3(a, b, dims=NN):
    ah, al = split(a)
    bh, bl = split(b)
    return dot(ah, bh, dims) + (dot(ah, bl, dims) + dot(al, bh, dims))


def rotated(c):
    half = c.shape[-1] // 2
    lane = lax.broadcasted_iota(jnp.int32, c.shape, c.ndim - 1)
    turned_c = pltpu.roll(c, half, c.ndim - 1)
    return jnp.where(lane < half, -turned_c, turned_c)


def lay_out(store, at, c):
    rows, cols = c.shape
    high, low = split(c)
    rhigh, rlow = split(rotated(c))
    store[at, :rows, :cols] = high
    store[at, :rows, cols:] = low
    store[at, rows:, :cols] = rhigh
    store[at, rows:, cols:] = rlow


def applied(mh, ml, b):
    cols = b.shape[1] // 2
    p = dot(mh, b)
    return p[:, :cols] + (p[:, cols:] + dot(ml, b[:, :cols]))


def masked(basis, rank):
    lane = lax.broadcasted_iota(jnp.int32, basis.shape, 1)
    return jnp.where(lane < rank, basis, 0.0)


def params(mb=48):
    return pltpu.CompilerParams(vmem_limit_bytes=mb * 1024 * 1024)


def cost(flops, nbytes):
    return pl.CostEstimate(flops=int(flops), bytes_accessed=int(nbytes), transcendentals=0)


def up_kernel(per, rank, cur, basis, transfer, coef, mid):
    step = pl.program_id(0)

    @pl.when(step == 0)
    def _():
        mid[...] = jnp.zeros_like(mid)

    total = mid[...]
    for i in range(per):
        c = dot3(masked(basis[i], rank[step * per + i]), cur[i], TN)
        coef[i] = c
        total += dot3(transfer[i], c, TN)
    mid[...] = total


def up(rank, cur, basis, transfer):
    leaves, panel, width = basis.shape
    cols = cur.shape[2]
    per = 4
    block = lambda a: pl.BlockSpec((per,) + a.shape[1:], lambda i: (i, 0, 0))
    return pl.pallas_call(
        functools.partial(up_kernel, per),
        grid=(leaves // per,),
        in_specs=[SMEM, block(cur), block(basis), block(transfer)],
        out_specs=[
            pl.BlockSpec((per, width, cols), lambda i: (i, 0, 0)),
            pl.BlockSpec((width, cols), lambda i: (0, 0)),
        ],
        out_shape=[
            jax.ShapeDtypeStruct((leaves, width, cols), F32),
            jax.ShapeDtypeStruct((width, cols), F32),
        ],
        compiler_params=params(),
        cost_estimate=cost(leaves * 12 * panel * width * cols, 16 * leaves * panel * width),
        name="up",
    )(rank, cur, basis, transfer)


def table_kernel(table, high, low):
    for i in range(table.shape[0]):
        h0, l0 = split(table[i, 0])
        h1, l1 = split(table[i, 1])
        w = h0.shape[1]
        high[i, :, :w] = h0
        high[i, :, w:] = h1
        low[i, :, :w] = l0
        low[i, :, w:] = l1


def split_table(table):
    kinds, two, a, b = table.shape
    per = 8 if kinds % 8 == 0 else 1
    out = pl.BlockSpec((per, a, 2 * b), lambda i: (i, 0, 0))
    return pl.pallas_call(
        table_kernel,
        grid=(kinds // per,),
        in_specs=[pl.BlockSpec((per, 2, a, b), lambda i: (i, 0, 0, 0))],
        out_specs=[out, out],
        out_shape=[jax.ShapeDtypeStruct((kinds, a, 2 * b), BF16)] * 2,
        compiler_params=params(),
        cost_estimate=cost(kinds * a * b * 20, kinds * a * b * 16),
        name="table",
    )(table)


UNROLL = 4


def far_kernel(nsrc, slots, first, index, *refs):
    coefs = refs[:nsrc]
    high, low = refs[nsrc], refs[nsrc + 1]
    at = nsrc + 2
    old = None
    if not first:
        old = refs[at]
        at += 1
    new, laid, order, acc = refs[at:]
    rows = new.shape[0]
    base = 0
    for c in coefs:
        @pl.loop(0, c.shape[0], unroll=2)
        def _(l, c=c, base=base):
            lay_out(laid, base + l, c[l])

        base += c.shape[0]
    if first:
        acc[...] = jnp.zeros_like(acc)
    else:
        acc[:rows] = old[...]

    def compact(i, count):
        order[0, count] = index[0, i]
        order[1, count] = index[1, i]
        order[2, count] = index[2, i]
        return count + jnp.where(index[2, i] >= 0, 1, 0)

    count = lax.fori_loop(0, slots, compact, 0)
    for u in range(UNROLL):
        order[0, count + u] = 0
        order[1, count + u] = 0
        order[2, count + u] = rows

    @pl.loop(0, (count + UNROLL - 1) // UNROLL)
    def _(i):
        results = []
        for u in range(UNROLL):
            k = order[1, i * UNROLL + u]
            results.append(applied(high[k], low[k], laid[order[0, i * UNROLL + u]]))
        for u in range(UNROLL):
            acc[order[2, i * UNROLL + u]] += results[u]

    new[...] = acc[:rows]


def far(index, coefs, tables, rows, old=None):
    slots = index.shape[1]
    width, cols = coefs[0].shape[1:]
    leaves = sum(c.shape[0] for c in coefs)
    first = old is None
    operands = [index, *coefs, *tables] + ([] if first else [old])
    kwargs = {} if first else {"input_output_aliases": {len(operands) - 1: 0}}
    return pl.pallas_call(
        functools.partial(far_kernel, len(coefs), slots, first),
        in_specs=[SMEM] + [VMEM] * (len(operands) - 1),
        out_specs=VMEM,
        out_shape=jax.ShapeDtypeStruct((rows, width, cols), F32),
        scratch_shapes=[
            pltpu.VMEM((leaves, 2 * width, 2 * cols), BF16),
            pltpu.SMEM((3, slots + UNROLL), jnp.int32),
            pltpu.VMEM((rows + 1, width, cols), F32),
        ],
        compiler_params=params(56),
        cost_estimate=cost(slots * 12 * width * width * cols, 12 * 2 ** 20),
        name="far",
        **kwargs,
    )(*operands)


def near_kernel(per, tgt, src, below, cur, above, blocks, out, laid):
    step = pl.program_id(0)

    @pl.when(step == 0)
    def _():
        out[...] = jnp.zeros_like(out)
        base = 0
        for part in (below, cur, above):
            @pl.loop(0, part.shape[0], unroll=2)
            def _(l, part=part, base=base):
                lay_out(laid, base + l, part[l])

            base += part.shape[0]

    results = []
    for u in range(per):
        h0, l0 = split(blocks[u, 0])
        h1, l1 = split(blocks[u, 1])
        b = laid[src[step * per + u]]
        results.append(
            applied(
                jnp.concatenate([h0, h1], axis=1), jnp.concatenate([l0, l1], axis=1), b
            )
        )
    for u in range(per):
        out[tgt[step * per + u]] += results[u]


def near(tgt, src, below, cur, above, blocks):
    count, two, a, b = blocks.shape
    leaves, panel, cols = cur.shape
    per = 4 if count % 4 == 0 else 1
    total = leaves + below.shape[0] + above.shape[0]
    whole = lambda x: pl.BlockSpec(x.shape, lambda i: (0,) * x.ndim)
    return pl.pallas_call(
        functools.partial(near_kernel, per),
        grid=(count // per,),
        in_specs=[
            SMEM,
            SMEM,
            whole(below),
            whole(cur),
            whole(above),
            pl.BlockSpec((per, two, a, b), lambda i: (i, 0, 0, 0)),
        ],
        out_specs=pl.BlockSpec((leaves, a, cols), lambda i: (0, 0, 0)),
        out_shape=jax.ShapeDtypeStruct((leaves, a, cols), F32),
        scratch_shapes=[pltpu.VMEM((total, 2 * b, 2 * cols), BF16)],
        compiler_params=params(),
        cost_estimate=cost(count * 12 * a * b * cols, count * 8 * a * b),
        name="near",
    )(tgt, src, below, cur, above, blocks)


def top_up_kernel(n, sub, *refs):
    packs, mids, out = refs[:n], refs[n : 2 * n], refs[2 * n]
    me = sub[0]
    rows = packs[0].shape[1]
    for d in range(n):
        total = None
        for e in range(n):
            part = dot3(packs[d][lax.rem(me - e + n, n)], mids[e][...])
            total = part if total is None else total + part
        q = lax.rem(me - d + n, n)
        out[pl.ds(pl.multiple_of(q * rows, rows), rows), :] = total


def top_up(sub, packs, mids):
    n = len(packs)
    return pl.pallas_call(
        functools.partial(top_up_kernel, n),
        in_specs=[SMEM] + [VMEM] * (2 * n),
        out_specs=VMEM,
        out_shape=jax.ShapeDtypeStruct(mids[0].shape, F32),
        compiler_params=params(),
        cost_estimate=cost(2e7, 2 ** 20),
        name="top_up",
    )(sub, *packs, *mids)


def top_down_kernel(n, sub, partner, *refs):
    packs, tops, out, field, transfer = refs[:n], refs[n], refs[n + 1], refs[n + 2], refs[n + 3]
    me = sub[0]
    rows = packs[0].shape[1]
    partners = [tops[partner[k]] for k in range(partner.shape[0])]
    turned_partners = [rotated(p) for p in partners]
    for d in range(n):
        total = jnp.zeros((rows, field.shape[1]), F32)
        for k in range(partner.shape[0]):
            total += dot3(packs[d][n + 2 * k], partners[k])
            total += dot3(packs[d][n + 2 * k + 1], turned_partners[k])
        q = lax.rem(me - d + n, n)
        span = pl.ds(pl.multiple_of(q * rows, rows), rows)
        field[span, :] = total
        transfer[span, :] = packs[d][me]
    out[...] = dot3(transfer[...], field[...], TN)


def top_down(sub, partner, packs, tops):
    n = len(packs)
    width, cols = tops.shape[1:]
    return pl.pallas_call(
        functools.partial(top_down_kernel, n),
        in_specs=[SMEM, SMEM] + [VMEM] * (n + 1),
        out_specs=VMEM,
        out_shape=jax.ShapeDtypeStruct((packs[0].shape[2], cols), F32),
        scratch_shapes=[pltpu.VMEM((width, cols), F32), pltpu.VMEM((width, packs[0].shape[2]), F32)],
        compiler_params=params(),
        cost_estimate=cost(4e7, 2 ** 20),
        name="top_down",
    )(sub, partner, *packs, tops)


def down_kernel(per, rank, own, below, above, near_part, transfer, basis, mid, out):
    step = pl.program_id(0)
    for i in range(per):
        field = own[i] + (below[i] + above[i]) + dot3(transfer[i], mid[...])
        out[i] = dot3(masked(basis[i], rank[step * per + i]), field) + near_part[i]


def down(rank, own, below, above, near_part, transfer, basis, mid):
    leaves, panel, width = basis.shape
    cols = mid.shape[1]
    per = 4
    block = lambda a: pl.BlockSpec((per,) + a.shape[1:], lambda i: (i, 0, 0))
    return pl.pallas_call(
        functools.partial(down_kernel, per),
        grid=(leaves // per,),
        in_specs=[SMEM]
        + [block(a) for a in (own, below, above, near_part, transfer, basis)]
        + [pl.BlockSpec(mid.shape, lambda i: (0, 0))],
        out_specs=pl.BlockSpec((per, panel, cols), lambda i: (i, 0, 0)),
        out_shape=jax.ShapeDtypeStruct((leaves, panel, cols), F32),
        compiler_params=params(),
        cost_estimate=cost(leaves * 12 * panel * width * cols, 28 * leaves * panel * width),
        name="down",
    )(rank, own, below, above, near_part, transfer, basis, mid)


def per_device(
    currents,
    leaf_basis,
    leaf_rank,
    leaf_transfer,
    top_transfer,
    far_table,
    send_src,
    recv_tgt,
    recv_type,
    top_coupling,
    top_list,
    near_blocks,
    near_tgt,
    near_src,
):
    leaves, panel, width = leaf_basis.shape
    cols = currents.shape[1]
    n = lax.axis_size("sub")
    me = lax.axis_index("sub")
    cur = currents.reshape(leaves, panel, cols)

    transfer_share = jnp.swapaxes(top_transfer[0], 1, 2)
    coupling_share = top_coupling[0].reshape((-1,) + top_coupling.shape[3:])
    packs = gather_sub(jnp.concatenate([transfer_share, coupling_share], axis=0))
    below_rim = shifted(cur[leaves - HALO_L :], ("leaf", "sub"), 1)
    above_rim = shifted(cur[:HALO_L], ("leaf", "sub"), -1)
    sends = gather_sub(send_src[0])
    recv = jnp.stack([recv_tgt[0], recv_type[0]])
    recv_below = shifted(recv[:, 2], "leaf", 1)
    recv_above = shifted(recv[:, 0], "leaf", -1)
    recv = jnp.stack([recv_below, recv[:, 1], recv_above], axis=1)

    coef, mid = up(leaf_rank, cur, leaf_basis, leaf_transfer)
    mids = gather_sub(mid)

    before = turned(coef, 1)
    after = turned(coef, -1)
    if n == 4:
        half = leaves // 2
        groups = [[coef], [before, after], [turned(before[:half], 1), turned(after[half:], -1)]]
        shifts = [[0], [1, n - 1], [2]]
    else:
        groups = [[turned(coef, d) if d else coef] for d in range(n)]
        shifts = [[d] for d in range(n)]

    def slots(ds):
        parts = []
        for at, d in enumerate(ds):
            source = lax.dynamic_index_in_dim(sends[d], me, 1, keepdims=False)
            q = lax.rem(me - d + n, n)
            info = lax.dynamic_index_in_dim(recv, q, 2, keepdims=False)
            parts.append(
                jnp.stack(
                    [
                        jnp.maximum(source, 0) + at * leaves,
                        info[1],
                        jnp.where(source >= 0, info[0], -1),
                    ]
                )
            )
        return jnp.concatenate(parts, axis=2)

    def indices(ds, offsets):
        info = slots(ds)
        picked = []
        for place, o in enumerate(offsets):
            t = info[2, o]
            picked.append(
                jnp.stack([info[0, o], info[1, o], jnp.where(t >= 0, t + place * leaves, -1)])
            )
        return jnp.concatenate(picked, axis=1)

    tables = split_table(far_table)
    outer = own = None
    for ds, coefs in zip(shifts, groups):
        outer = far(indices(ds, (0, 2)), coefs, tables, 2 * leaves, outer)
        own = far(indices(ds, (1,)), coefs, tables, leaves, own)
    from_above = shifted(outer[:leaves], "leaf", -1)
    from_below = shifted(outer[leaves:], "leaf", 1)

    near_part = near(near_tgt[0], near_src[0], below_rim, cur, above_rim, near_blocks)

    sub = me.reshape(1).astype(jnp.int32)
    top = top_up(sub, packs, mids)
    tops = lax.all_gather(top, "leaf", axis=0)
    mid_field = top_down(sub, top_list[0], packs, tops)

    out = down(
        leaf_rank, own, from_below, from_above, near_part, leaf_transfer, leaf_basis, mid_field
    )
    return out.reshape(leaves * panel, cols)


def solution(mesh):
    placed = (
        P(("leaf", "sub"), None),
        P(("leaf", "sub"), None, None),
        P(("leaf", "sub")),
        P(("leaf", "sub"), None, None),
        P("leaf", None, None, "sub"),
        P(),
        P(("leaf", "sub"), None, None, None),
        P(("leaf", "sub"), None, None, None),
        P(("leaf", "sub"), None, None, None),
        P("leaf", None, None, "sub", None),
        P("leaf", None),
        P(("leaf", "sub"), None, None, None),
        P(("leaf", "sub"), None),
        P(("leaf", "sub"), None),
    )
    return jax.shard_map(
        per_device, mesh=mesh, in_specs=placed, out_specs=P(("leaf", "sub"), None), check_vma=False
    )
```

```python
import functools

import jax
import jax.numpy as jnp
from jax import lax
from jax.experimental import pallas as pl
from jax.experimental.pallas import tpu as pltpu
from jax.sharding import PartitionSpec as P

HALO_L = 4
F32 = jnp.float32
BF16 = jnp.bfloat16
NN = (((1,), (0,)), ((), ()))
TN = (((0,), (0,)), ((), ()))


SMEM = pl.BlockSpec(memory_space=pltpu.SMEM)
VMEM = pl.BlockSpec(memory_space=pltpu.VMEM)


def shifted(value, axis, by):
    length = lax.axis_size(axis)
    pairs = [(i, i + by) for i in range(length) if 0 <= i + by < length]
    return lax.ppermute(value, axis, pairs)


def turned(value, by):
    length = lax.axis_size("sub")
    return lax.ppermute(value, "sub", [(i, (i + by) % length) for i in range(length)])


def gather_sub(value):
    return [value] + [turned(value, d) for d in range(1, lax.axis_size("sub"))]


def split(x):
    high = x.astype(BF16)
    return high, (x - high.astype(F32)).astype(BF16)


def dot(a, b, dims=NN):
    return lax.dot_general(a, b, dims, preferred_element_type=F32)


def dot3(a, b, dims=NN):
    ah, al = split(a)
    bh, bl = split(b)
    return dot(ah, bh, dims) + (dot(ah, bl, dims) + dot(al, bh, dims))


def rotated(c):
    half = c.shape[-1] // 2
    lane = lax.broadcasted_iota(jnp.int32, c.shape, c.ndim - 1)
    turned_c = pltpu.roll(c, half, c.ndim - 1)
    return jnp.where(lane < half, -turned_c, turned_c)


def lay_out(store, at, c):
    rows, cols = c.shape
    high, low = split(c)
    rhigh, rlow = split(rotated(c))
    store[at, :rows, :cols] = high
    store[at, :rows, cols:] = low
    store[at, rows:, :cols] = rhigh
    store[at, rows:, cols:] = rlow


def applied(mh, ml, b):
    cols = b.shape[1] // 2
    p = dot(mh, b)
    return p[:, :cols] + (p[:, cols:] + dot(ml, b[:, :cols]))


def masked(basis, rank):
    lane = lax.broadcasted_iota(jnp.int32, basis.shape, 1)
    return jnp.where(lane < rank, basis, 0.0)


def params(mb=48):
    return pltpu.CompilerParams(vmem_limit_bytes=mb * 1024 * 1024)


def cost(flops, nbytes):
    return pl.CostEstimate(flops=int(flops), bytes_accessed=int(nbytes), transcendentals=0)


def up_kernel(per, rank, cur, basis, transfer, coef, mid):
    step = pl.program_id(0)

    @pl.when(step == 0)
    def _():
        mid[...] = jnp.zeros_like(mid)

    total = mid[...]
    for i in range(per):
        c = dot3(masked(basis[i], rank[step * per + i]), cur[i], TN)
        coef[i] = c
        total += dot3(transfer[i], c, TN)
    mid[...] = total


def up(rank, cur, basis, transfer):
    leaves, panel, width = basis.shape
    cols = cur.shape[2]
    per = 4
    block = lambda a: pl.BlockSpec((per,) + a.shape[1:], lambda i: (i, 0, 0))
    return pl.pallas_call(
        functools.partial(up_kernel, per),
        grid=(leaves // per,),
        in_specs=[SMEM, block(cur), block(basis), block(transfer)],
        out_specs=[
            pl.BlockSpec((per, width, cols), lambda i: (i, 0, 0)),
            pl.BlockSpec((width, cols), lambda i: (0, 0)),
        ],
        out_shape=[
            jax.ShapeDtypeStruct((leaves, width, cols), F32),
            jax.ShapeDtypeStruct((width, cols), F32),
        ],
        compiler_params=params(),
        cost_estimate=cost(leaves * 12 * panel * width * cols, 16 * leaves * panel * width),
        name="up",
    )(rank, cur, basis, transfer)


def table_kernel(table, high, low):
    for i in range(table.shape[0]):
        h0, l0 = split(table[i, 0])
        h1, l1 = split(table[i, 1])
        w = h0.shape[1]
        high[i, :, :w] = h0
        high[i, :, w:] = h1
        low[i, :, :w] = l0
        low[i, :, w:] = l1


def split_table(table):
    kinds, two, a, b = table.shape
    per = 8 if kinds % 8 == 0 else 1
    out = pl.BlockSpec((per, a, 2 * b), lambda i: (i, 0, 0))
    return pl.pallas_call(
        table_kernel,
        grid=(kinds // per,),
        in_specs=[pl.BlockSpec((per, 2, a, b), lambda i: (i, 0, 0, 0))],
        out_specs=[out, out],
        out_shape=[jax.ShapeDtypeStruct((kinds, a, 2 * b), BF16)] * 2,
        compiler_params=params(),
        cost_estimate=cost(kinds * a * b * 20, kinds * a * b * 16),
        name="table",
    )(table)


UNROLL = 4


def far_kernel(n, moves, offsets, span, first, me_ref, recv, *refs):
    count_moves = len(moves)
    sends, refs = refs[:count_moves], refs[count_moves:]
    coefs, refs = refs[:count_moves], refs[count_moves:]
    high, low, refs = refs[0], refs[1], refs[2:]
    old = None
    if not first:
        old, refs = refs[0], refs[1:]
    new, laid, order, acc = refs
    rows = new.shape[0]
    me = me_ref[0]
    leaves = coefs[0].shape[0]
    cap = recv.shape[3]
    if first:
        acc[...] = jnp.zeros_like(acc)
    else:
        acc[:rows] = old[...]
    count = 0
    for at, move in enumerate(moves):
        q = me - move
        here = (q >= 0) & (q < n)
        peer = jnp.clip(q, 0, n - 1)

        @pl.when(here)
        def _(at=at):
            @pl.loop(0, leaves, unroll=2)
            def _(l):
                lay_out(laid, at * leaves + l, coefs[at][l])

        for place, o in enumerate(offsets):
            def compact(j, count, at=at, o=o, place=place, here=here, peer=peer):
                source = sends[at][o, me, j]
                order[0, count] = source + at * leaves
                order[1, count] = recv[1, o, peer, j]
                order[2, count] = recv[0, o, peer, j] + place * leaves
                return count + jnp.where((source >= 0) & here, 1, 0)

            count = lax.fori_loop(0, cap, compact, count)
    for u in range(UNROLL):
        order[0, count + u] = order[0, 0] * 0
        order[1, count + u] = 0
        order[2, count + u] = rows

    @pl.loop(0, (count + UNROLL - 1) // UNROLL)
    def _(i):
        results = []
        for u in range(UNROLL):
            k = order[1, i * UNROLL + u]
            results.append(applied(high[k], low[k], laid[order[0, i * UNROLL + u]]))
        for u in range(UNROLL):
            acc[order[2, i * UNROLL + u]] += results[u]

    new[...] = acc[:rows]


def far(me, recv, moves, sends, coefs, tables, n, offsets, old=None):
    leaves, width, cols = coefs[0].shape
    rows = len(offsets) * leaves
    slots = len(moves) * len(offsets) * recv.shape[3]
    first = old is None
    operands = [me, recv, *sends, *coefs, *tables] + ([] if first else [old])
    kwargs = {} if first else {"input_output_aliases": {len(operands) - 1: 0}}
    smems = 2 + len(sends)
    return pl.pallas_call(
        functools.partial(far_kernel, n, moves, offsets, leaves, first),
        in_specs=[SMEM] * smems + [VMEM] * (len(operands) - smems),
        out_specs=VMEM,
        out_shape=jax.ShapeDtypeStruct((rows, width, cols), F32),
        scratch_shapes=[
            pltpu.VMEM((len(moves) * leaves, 2 * width, 2 * cols), BF16),
            pltpu.SMEM((3, slots + UNROLL), jnp.int32),
            pltpu.VMEM((rows + 1, width, cols), F32),
        ],
        compiler_params=params(56),
        cost_estimate=cost(slots * 12 * width * width * cols, 12 * 2 ** 20),
        name="far",
        **kwargs,
    )(*operands)


def near_kernel(per, tgt, src, below, cur, above, blocks, out, laid):
    step = pl.program_id(0)

    @pl.when(step == 0)
    def _():
        out[...] = jnp.zeros_like(out)
        base = 0
        for part in (below, cur, above):
            @pl.loop(0, part.shape[0], unroll=2)
            def _(l, part=part, base=base):
                lay_out(laid, base + l, part[l])

            base += part.shape[0]

    results = []
    for u in range(per):
        h0, l0 = split(blocks[u, 0])
        h1, l1 = split(blocks[u, 1])
        b = laid[src[step * per + u]]
        results.append(
            applied(
                jnp.concatenate([h0, h1], axis=1), jnp.concatenate([l0, l1], axis=1), b
            )
        )
    for u in range(per):
        out[tgt[step * per + u]] += results[u]


def near(tgt, src, below, cur, above, blocks):
    count, two, a, b = blocks.shape
    leaves, panel, cols = cur.shape
    per = 4 if count % 4 == 0 else 1
    total = leaves + below.shape[0] + above.shape[0]
    whole = lambda x: pl.BlockSpec(x.shape, lambda i: (0,) * x.ndim)
    return pl.pallas_call(
        functools.partial(near_kernel, per),
        grid=(count // per,),
        in_specs=[
            SMEM,
            SMEM,
            whole(below),
            whole(cur),
            whole(above),
            pl.BlockSpec((per, two, a, b), lambda i: (i, 0, 0, 0)),
        ],
        out_specs=pl.BlockSpec((leaves, a, cols), lambda i: (0, 0, 0)),
        out_shape=jax.ShapeDtypeStruct((leaves, a, cols), F32),
        scratch_shapes=[pltpu.VMEM((total, 2 * b, 2 * cols), BF16)],
        compiler_params=params(),
        cost_estimate=cost(count * 12 * a * b * cols, count * 8 * a * b),
        name="near",
    )(tgt, src, below, cur, above, blocks)


def top_up_kernel(n, sub, *refs):
    packs, mids, out = refs[:n], refs[n : 2 * n], refs[2 * n]
    me = sub[0]
    rows = packs[0].shape[1]
    for d in range(n):
        total = None
        for e in range(n):
            part = dot3(packs[d][lax.rem(me - e + n, n)], mids[e][...])
            total = part if total is None else total + part
        q = lax.rem(me - d + n, n)
        out[pl.ds(pl.multiple_of(q * rows, rows), rows), :] = total


def top_up(sub, packs, mids):
    n = len(packs)
    return pl.pallas_call(
        functools.partial(top_up_kernel, n),
        in_specs=[SMEM] + [VMEM] * (2 * n),
        out_specs=VMEM,
        out_shape=jax.ShapeDtypeStruct(mids[0].shape, F32),
        compiler_params=params(),
        cost_estimate=cost(2e7, 2 ** 20),
        name="top_up",
    )(sub, *packs, *mids)


def top_down_kernel(n, sub, partner, *refs):
    packs, tops, out, field, transfer = refs[:n], refs[n], refs[n + 1], refs[n + 2], refs[n + 3]
    me = sub[0]
    rows = packs[0].shape[1]
    partners = [tops[partner[k]] for k in range(partner.shape[0])]
    turned_partners = [rotated(p) for p in partners]
    for d in range(n):
        total = jnp.zeros((rows, field.shape[1]), F32)
        for k in range(partner.shape[0]):
            total += dot3(packs[d][n + 2 * k], partners[k])
            total += dot3(packs[d][n + 2 * k + 1], turned_partners[k])
        q = lax.rem(me - d + n, n)
        span = pl.ds(pl.multiple_of(q * rows, rows), rows)
        field[span, :] = total
        transfer[span, :] = packs[d][me]
    out[...] = dot3(transfer[...], field[...], TN)


def top_down(sub, partner, packs, tops):
    n = len(packs)
    width, cols = tops.shape[1:]
    return pl.pallas_call(
        functools.partial(top_down_kernel, n),
        in_specs=[SMEM, SMEM] + [VMEM] * (n + 1),
        out_specs=VMEM,
        out_shape=jax.ShapeDtypeStruct((packs[0].shape[2], cols), F32),
        scratch_shapes=[pltpu.VMEM((width, cols), F32), pltpu.VMEM((width, packs[0].shape[2]), F32)],
        compiler_params=params(),
        cost_estimate=cost(4e7, 2 ** 20),
        name="top_down",
    )(sub, partner, *packs, tops)


def down_kernel(per, rank, own, below, above, near_part, transfer, basis, mid, out):
    step = pl.program_id(0)
    for i in range(per):
        field = own[i] + (below[i] + above[i]) + dot3(transfer[i], mid[...])
        out[i] = dot3(masked(basis[i], rank[step * per + i]), field) + near_part[i]


def down(rank, own, below, above, near_part, transfer, basis, mid):
    leaves, panel, width = basis.shape
    cols = mid.shape[1]
    per = 4
    block = lambda a: pl.BlockSpec((per,) + a.shape[1:], lambda i: (i, 0, 0))
    return pl.pallas_call(
        functools.partial(down_kernel, per),
        grid=(leaves // per,),
        in_specs=[SMEM]
        + [block(a) for a in (own, below, above, near_part, transfer, basis)]
        + [pl.BlockSpec(mid.shape, lambda i: (0, 0))],
        out_specs=pl.BlockSpec((per, panel, cols), lambda i: (i, 0, 0)),
        out_shape=jax.ShapeDtypeStruct((leaves, panel, cols), F32),
        compiler_params=params(),
        cost_estimate=cost(leaves * 12 * panel * width * cols, 28 * leaves * panel * width),
        name="down",
    )(rank, own, below, above, near_part, transfer, basis, mid)


def per_device(
    currents,
    leaf_basis,
    leaf_rank,
    leaf_transfer,
    top_transfer,
    far_table,
    send_src,
    recv_tgt,
    recv_type,
    top_coupling,
    top_list,
    near_blocks,
    near_tgt,
    near_src,
):
    leaves, panel, width = leaf_basis.shape
    cols = currents.shape[1]
    n = lax.axis_size("sub")
    me = lax.axis_index("sub")
    cur = currents.reshape(leaves, panel, cols)

    transfer_share = jnp.swapaxes(top_transfer[0], 1, 2)
    coupling_share = top_coupling[0].reshape((-1,) + top_coupling.shape[3:])
    packs = gather_sub(jnp.concatenate([transfer_share, coupling_share], axis=0))
    below_rim = shifted(cur[leaves - HALO_L :], ("leaf", "sub"), 1)
    above_rim = shifted(cur[:HALO_L], ("leaf", "sub"), -1)
    sends = gather_sub(send_src[0])
    recv = jnp.stack([recv_tgt[0], recv_type[0]])
    recv_below = shifted(recv[:, 2], "leaf", 1)
    recv_above = shifted(recv[:, 0], "leaf", -1)
    recv = jnp.stack([recv_below, recv[:, 1], recv_above], axis=1)

    coef, mid = up(leaf_rank, cur, leaf_basis, leaf_transfer)
    below, above = coef, coef
    below_next, above_next = shifted(below, "sub", 1), shifted(above, "sub", -1)
    mids = gather_sub(mid)
    me1 = me.reshape(1).astype(jnp.int32)
    tables = split_table(far_table)
    both = (0, 1, 2)
    field = far(me1, recv, (0,), [sends[0]], [coef], tables, n, both)
    near_part = near_in = None
    mid_field = None
    for move in range(1, n):
        field, below, above = lax.optimization_barrier((field, below_next, above_next))
        if move == n - 2:
            below, above, *rest = lax.optimization_barrier((below, above, *mids, *packs))
            mids, packs = rest[:n], rest[n:]
        if move == n - 1:
            below, above, mid_field = lax.optimization_barrier((below, above, mid_field))
        args = (me1, recv, (move, -move), [sends[move], sends[(n - move) % n]], [below, above], tables, n)
        if move < n - 1:
            below_next, above_next = shifted(below, "sub", 1), shifted(above, "sub", -1)
            field = far(*args, both, field)
            if move == 1:
                cur_in, below, above = lax.optimization_barrier((cur, below, above))
                near_part = near(near_tgt[0], near_src[0], below_rim, cur_in, above_rim, near_blocks)
                below_next, above_next, near_part = lax.optimization_barrier(
                    (below_next, above_next, near_part)
                )
            if move == n - 2:
                top = top_up(me1, packs, mids)
                tops = lax.all_gather(top, "leaf", axis=0)
                mid_field = top_down(me1, top_list[0], packs, tops)
        else:
            outer = jnp.concatenate([field[:leaves], field[2 * leaves :]], axis=0)
            outer = far(*args, (0, 2), outer)
            from_above = shifted(outer[:leaves], "leaf", -1)
            from_below = shifted(outer[leaves:], "leaf", 1)
            own = far(*args, (1,), field[leaves : 2 * leaves])

    out = down(
        leaf_rank, own, from_below, from_above, near_part, leaf_transfer, leaf_basis, mid_field
    )
    return out.reshape(leaves * panel, cols)


def solution(mesh):
    placed = (
        P(("leaf", "sub"), None),
        P(("leaf", "sub"), None, None),
        P(("leaf", "sub")),
        P(("leaf", "sub"), None, None),
        P("leaf", None, None, "sub"),
        P(),
        P(("leaf", "sub"), None, None, None),
        P(("leaf", "sub"), None, None, None),
        P(("leaf", "sub"), None, None, None),
        P("leaf", None, None, "sub", None),
        P("leaf", None),
        P(("leaf", "sub"), None, None, None),
        P(("leaf", "sub"), None),
        P(("leaf", "sub"), None),
    )
    return jax.shard_map(
        per_device, mesh=mesh, in_specs=placed, out_specs=P(("leaf", "sub"), None), check_vma=False
    )
```

```python
import functools

import jax
import jax.numpy as jnp
from jax import lax
from jax.experimental import pallas as pl
from jax.experimental.pallas import tpu as pltpu
from jax.sharding import PartitionSpec as P

HALO_L = 4
F32 = jnp.float32
BF16 = jnp.bfloat16
NN = (((1,), (0,)), ((), ()))
TN = (((0,), (0,)), ((), ()))


SMEM = pl.BlockSpec(memory_space=pltpu.SMEM)
VMEM = pl.BlockSpec(memory_space=pltpu.VMEM)


def shifted(value, axis, by):
    length = lax.axis_size(axis)
    pairs = [(i, i + by) for i in range(length) if 0 <= i + by < length]
    return lax.ppermute(value, axis, pairs)


def turned(value, by):
    length = lax.axis_size("sub")
    return lax.ppermute(value, "sub", [(i, (i + by) % length) for i in range(length)])


def gather_sub(value):
    return [value] + [turned(value, d) for d in range(1, lax.axis_size("sub"))]


def split(x):
    high = x.astype(BF16)
    return high, (x - high.astype(F32)).astype(BF16)


def dot(a, b, dims=NN):
    return lax.dot_general(a, b, dims, preferred_element_type=F32)


def dot3(a, b, dims=NN):
    ah, al = split(a)
    bh, bl = split(b)
    return dot(ah, bh, dims) + (dot(ah, bl, dims) + dot(al, bh, dims))


def rotated(c):
    half = c.shape[-1] // 2
    lane = lax.broadcasted_iota(jnp.int32, c.shape, c.ndim - 1)
    turned_c = pltpu.roll(c, half, c.ndim - 1)
    return jnp.where(lane < half, -turned_c, turned_c)


def lay_out(store, at, c):
    rows, cols = c.shape
    high, low = split(c)
    rhigh, rlow = split(rotated(c))
    store[at, :rows, :cols] = high
    store[at, :rows, cols:] = low
    store[at, rows:, :cols] = rhigh
    store[at, rows:, cols:] = rlow


def applied(mh, ml, b):
    cols = b.shape[1] // 2
    p = dot(mh, b)
    return p[:, :cols] + (p[:, cols:] + dot(ml, b[:, :cols]))


def masked(basis, rank):
    lane = lax.broadcasted_iota(jnp.int32, basis.shape, 1)
    return jnp.where(lane < rank, basis, 0.0)


def params(mb=48):
    return pltpu.CompilerParams(vmem_limit_bytes=mb * 1024 * 1024)


def cost(flops, nbytes):
    return pl.CostEstimate(flops=int(flops), bytes_accessed=int(nbytes), transcendentals=0)


def up_kernel(per, rank, cur, basis, transfer, coef, mid):
    step = pl.program_id(0)

    @pl.when(step == 0)
    def _():
        mid[...] = jnp.zeros_like(mid)

    total = mid[...]
    for i in range(per):
        c = dot3(masked(basis[i], rank[step * per + i]), cur[i], TN)
        coef[i] = c
        total += dot3(transfer[i], c, TN)
    mid[...] = total


def up(rank, cur, basis, transfer):
    leaves, panel, width = basis.shape
    cols = cur.shape[2]
    per = 4
    block = lambda a: pl.BlockSpec((per,) + a.shape[1:], lambda i: (i, 0, 0))
    return pl.pallas_call(
        functools.partial(up_kernel, per),
        grid=(leaves // per,),
        in_specs=[SMEM, block(cur), block(basis), block(transfer)],
        out_specs=[
            pl.BlockSpec((per, width, cols), lambda i: (i, 0, 0)),
            pl.BlockSpec((width, cols), lambda i: (0, 0)),
        ],
        out_shape=[
            jax.ShapeDtypeStruct((leaves, width, cols), F32),
            jax.ShapeDtypeStruct((width, cols), F32),
        ],
        compiler_params=params(),
        cost_estimate=cost(leaves * 12 * panel * width * cols, 16 * leaves * panel * width),
        name="up",
    )(rank, cur, basis, transfer)


def table_kernel(table, high, low):
    for i in range(table.shape[0]):
        h0, l0 = split(table[i, 0])
        h1, l1 = split(table[i, 1])
        w = h0.shape[1]
        high[i, :, :w] = h0
        high[i, :, w:] = h1
        low[i, :, :w] = l0
        low[i, :, w:] = l1


def split_table(table):
    kinds, two, a, b = table.shape
    per = 8 if kinds % 8 == 0 else 1
    out = pl.BlockSpec((per, a, 2 * b), lambda i: (i, 0, 0))
    return pl.pallas_call(
        table_kernel,
        grid=(kinds // per,),
        in_specs=[pl.BlockSpec((per, 2, a, b), lambda i: (i, 0, 0, 0))],
        out_specs=[out, out],
        out_shape=[jax.ShapeDtypeStruct((kinds, a, 2 * b), BF16)] * 2,
        compiler_params=params(),
        cost_estimate=cost(kinds * a * b * 20, kinds * a * b * 16),
        name="table",
    )(table)


UNROLL = 4


def far_kernel(n, moves, offsets, span, first, me_ref, recv, *refs):
    count_moves = len(moves)
    sends, refs = refs[:count_moves], refs[count_moves:]
    coefs, refs = refs[:count_moves], refs[count_moves:]
    high, low, refs = refs[0], refs[1], refs[2:]
    old = None
    if not first:
        old, refs = refs[0], refs[1:]
    outs, (laid, order, acc) = refs[:-3], refs[-3:]
    rows = acc.shape[0] - 1
    me = me_ref[0]
    leaves = coefs[0].shape[0]
    cap = recv.shape[3]
    if first:
        acc[...] = jnp.zeros_like(acc)
    elif old.shape[0] == rows:
        acc[:rows] = old[...]
    else:
        for place, o in enumerate(offsets):
            acc[place * span : (place + 1) * span] = old[o * span : (o + 1) * span]
    count = 0
    for at, move in enumerate(moves):
        q = me - move
        here = (q >= 0) & (q < n)
        peer = jnp.clip(q, 0, n - 1)

        @pl.when(here)
        def _(at=at):
            @pl.loop(0, leaves, unroll=2)
            def _(l):
                lay_out(laid, at * leaves + l, coefs[at][l])

        for place, o in enumerate(offsets):
            def compact(j, count, at=at, o=o, place=place, here=here, peer=peer):
                source = sends[at][o, me, j]
                order[0, count] = source + at * leaves
                order[1, count] = recv[1, o, peer, j]
                order[2, count] = recv[0, o, peer, j] + place * leaves
                return count + jnp.where((source >= 0) & here, 1, 0)

            count = lax.fori_loop(0, cap, compact, count)
    for u in range(UNROLL):
        order[0, count + u] = order[0, 0] * 0
        order[1, count + u] = 0
        order[2, count + u] = rows

    @pl.loop(0, (count + UNROLL - 1) // UNROLL)
    def _(i):
        results = []
        for u in range(UNROLL):
            k = order[1, i * UNROLL + u]
            results.append(applied(high[k], low[k], laid[order[0, i * UNROLL + u]]))
        for u in range(UNROLL):
            acc[order[2, i * UNROLL + u]] += results[u]

    each = rows // len(outs)
    for place, out in enumerate(outs):
        out[...] = acc[place * each : (place + 1) * each]


def far(me, recv, moves, sends, coefs, tables, n, offsets, old=None, outs=1):
    leaves, width, cols = coefs[0].shape
    rows = len(offsets) * leaves
    slots = len(moves) * len(offsets) * recv.shape[3]
    first = old is None
    operands = [me, recv, *sends, *coefs, *tables] + ([] if first else [old])
    alias = outs == 1 and not first and old.shape[0] == rows
    kwargs = {"input_output_aliases": {len(operands) - 1: 0}} if alias else {}
    smems = 2 + len(sends)
    return pl.pallas_call(
        functools.partial(far_kernel, n, moves, offsets, leaves, first),
        in_specs=[SMEM] * smems + [VMEM] * (len(operands) - smems),
        out_specs=[VMEM] * outs,
        out_shape=[jax.ShapeDtypeStruct((rows // outs, width, cols), F32)] * outs,
        scratch_shapes=[
            pltpu.VMEM((len(moves) * leaves, 2 * width, 2 * cols), BF16),
            pltpu.SMEM((3, slots + UNROLL), jnp.int32),
            pltpu.VMEM((rows + 1, width, cols), F32),
        ],
        compiler_params=params(56),
        cost_estimate=cost(slots * 12 * width * width * cols, 12 * 2 ** 20),
        name="far",
        **kwargs,
    )(*operands)


def near_kernel(per, tgt, src, below, cur, above, blocks, out, laid):
    step = pl.program_id(0)

    @pl.when(step == 0)
    def _():
        out[...] = jnp.zeros_like(out)
        base = 0
        for part in (below, cur, above):
            @pl.loop(0, part.shape[0], unroll=2)
            def _(l, part=part, base=base):
                lay_out(laid, base + l, part[l])

            base += part.shape[0]

    results = []
    for u in range(per):
        h0, l0 = split(blocks[u, 0])
        h1, l1 = split(blocks[u, 1])
        b = laid[src[step * per + u]]
        results.append(
            applied(
                jnp.concatenate([h0, h1], axis=1), jnp.concatenate([l0, l1], axis=1), b
            )
        )
    for u in range(per):
        out[tgt[step * per + u]] += results[u]


def near(tgt, src, below, cur, above, blocks):
    count, two, a, b = blocks.shape
    leaves, panel, cols = cur.shape
    per = 4 if count % 4 == 0 else 1
    total = leaves + below.shape[0] + above.shape[0]
    whole = lambda x: pl.BlockSpec(x.shape, lambda i: (0,) * x.ndim)
    return pl.pallas_call(
        functools.partial(near_kernel, per),
        grid=(count // per,),
        in_specs=[
            SMEM,
            SMEM,
            whole(below),
            whole(cur),
            whole(above),
            pl.BlockSpec((per, two, a, b), lambda i: (i, 0, 0, 0)),
        ],
        out_specs=pl.BlockSpec((leaves, a, cols), lambda i: (0, 0, 0)),
        out_shape=jax.ShapeDtypeStruct((leaves, a, cols), F32),
        scratch_shapes=[pltpu.VMEM((total, 2 * b, 2 * cols), BF16)],
        compiler_params=params(),
        cost_estimate=cost(count * 12 * a * b * cols, count * 8 * a * b),
        name="near",
    )(tgt, src, below, cur, above, blocks)


def top_up_kernel(n, held, sub, *refs):
    packs, out = refs[:n], refs[n]
    me = sub[0]
    rows, cols = packs[0].shape[1:]
    mids = [
        packs[e][n + held : 2 * n + held].reshape(n * rows, cols) for e in range(n)
    ]
    for d in range(n):
        total = None
        for e in range(n):
            part = dot3(packs[d][lax.rem(me - e + n, n)], mids[e])
            total = part if total is None else total + part
        q = lax.rem(me - d + n, n)
        out[pl.ds(pl.multiple_of(q * rows, rows), rows), :] = total


def top_up(sub, packs, held):
    n = len(packs)
    rows, cols = packs[0].shape[1:]
    return pl.pallas_call(
        functools.partial(top_up_kernel, n, held),
        in_specs=[SMEM] + [VMEM] * n,
        out_specs=VMEM,
        out_shape=jax.ShapeDtypeStruct((n * rows, cols), F32),
        compiler_params=params(),
        cost_estimate=cost(2e7, 2 ** 20),
        name="top_up",
    )(sub, *packs)


def top_down_kernel(n, sub, partner, *refs):
    packs, tops, out, field, transfer = refs[:n], refs[n], refs[n + 1], refs[n + 2], refs[n + 3]
    me = sub[0]
    rows = packs[0].shape[1]
    partners = [tops[partner[k]] for k in range(partner.shape[0])]
    turned_partners = [rotated(p) for p in partners]
    for d in range(n):
        total = jnp.zeros((rows, field.shape[1]), F32)
        for k in range(partner.shape[0]):
            total += dot3(packs[d][n + 2 * k], partners[k])
            total += dot3(packs[d][n + 2 * k + 1], turned_partners[k])
        q = lax.rem(me - d + n, n)
        span = pl.ds(pl.multiple_of(q * rows, rows), rows)
        field[span, :] = total
        transfer[span, :] = packs[d][me]
    out[...] = dot3(transfer[...], field[...], TN)


def top_down(sub, partner, packs, tops):
    n = len(packs)
    width, cols = tops.shape[1:]
    return pl.pallas_call(
        functools.partial(top_down_kernel, n),
        in_specs=[SMEM, SMEM] + [VMEM] * (n + 1),
        out_specs=VMEM,
        out_shape=jax.ShapeDtypeStruct((packs[0].shape[2], cols), F32),
        scratch_shapes=[pltpu.VMEM((width, cols), F32), pltpu.VMEM((width, packs[0].shape[2]), F32)],
        compiler_params=params(),
        cost_estimate=cost(4e7, 2 ** 20),
        name="top_down",
    )(sub, partner, *packs, tops)


def down_kernel(per, rank, own, below, above, near_part, transfer, basis, mid, out):
    step = pl.program_id(0)
    for i in range(per):
        field = own[i] + (below[i] + above[i]) + dot3(transfer[i], mid[...])
        out[i] = dot3(masked(basis[i], rank[step * per + i]), field) + near_part[i]


def down(rank, own, below, above, near_part, transfer, basis, mid):
    leaves, panel, width = basis.shape
    cols = mid.shape[1]
    per = 4
    block = lambda a: pl.BlockSpec((per,) + a.shape[1:], lambda i: (i, 0, 0))
    return pl.pallas_call(
        functools.partial(down_kernel, per),
        grid=(leaves // per,),
        in_specs=[SMEM]
        + [block(a) for a in (own, below, above, near_part, transfer, basis)]
        + [pl.BlockSpec(mid.shape, lambda i: (0, 0))],
        out_specs=pl.BlockSpec((per, panel, cols), lambda i: (i, 0, 0)),
        out_shape=jax.ShapeDtypeStruct((leaves, panel, cols), F32),
        compiler_params=params(),
        cost_estimate=cost(leaves * 12 * panel * width * cols, 28 * leaves * panel * width),
        name="down",
    )(rank, own, below, above, near_part, transfer, basis, mid)


def per_device(
    currents,
    leaf_basis,
    leaf_rank,
    leaf_transfer,
    top_transfer,
    far_table,
    send_src,
    recv_tgt,
    recv_type,
    top_coupling,
    top_list,
    near_blocks,
    near_tgt,
    near_src,
):
    leaves, panel, width = leaf_basis.shape
    cols = currents.shape[1]
    n = lax.axis_size("sub")
    me = lax.axis_index("sub")
    cur = currents.reshape(leaves, panel, cols)

    transfer_share = jnp.swapaxes(top_transfer[0], 1, 2)
    coupling_share = top_coupling[0].reshape((-1,) + top_coupling.shape[3:])
    below_rim = shifted(cur[leaves - HALO_L :], ("leaf", "sub"), 1)
    above_rim = shifted(cur[:HALO_L], ("leaf", "sub"), -1)
    recv = jnp.stack([recv_tgt[0], recv_type[0]])
    recv_below = shifted(recv[:, 2], "leaf", 1)
    recv_above = shifted(recv[:, 0], "leaf", -1)
    recv = jnp.stack([recv_below, recv[:, 1], recv_above], axis=1)

    coef, mid = up(leaf_rank, cur, leaf_basis, leaf_transfer)
    below, above = coef, coef
    below_next, above_next = shifted(below, "sub", 1), shifted(above, "sub", -1)
    share = transfer_share.shape[1]
    flat = send_src[0].reshape(-1).astype(F32)
    size = share * width
    blocks = -(-flat.shape[0] // size)
    flat = jnp.pad(flat, (0, blocks * size - flat.shape[0])).reshape(blocks, share, width)
    packs = gather_sub(
        jnp.concatenate([transfer_share, coupling_share, mid.reshape(-1, share, cols), flat], axis=0)
    )
    count = send_src[0].size
    sends = [send_src[0]] + [
        p[-blocks:].reshape(-1)[:count].astype(jnp.int32).reshape(send_src.shape[1:])
        for p in packs[1:]
    ]
    me1 = me.reshape(1).astype(jnp.int32)
    tables = split_table(far_table)
    both = (0, 1, 2)
    (field,) = far(me1, recv, (0,), [send_src[0]], [coef], tables, n, both)
    near_part = near_in = None
    mid_field = None
    for move in range(1, n):
        field, below, above = lax.optimization_barrier((field, below_next, above_next))
        if move == n - 2:
            below, above, *packs = lax.optimization_barrier((below, above, *packs))
        if move == n - 1:
            below, above, mid_field, near_part = lax.optimization_barrier(
                (below, above, mid_field, near_part)
            )
        args = (me1, recv, (move, -move), [sends[move], sends[(n - move) % n]], [below, above], tables, n)
        if move < n - 1:
            below_next, above_next = shifted(below, "sub", 1), shifted(above, "sub", -1)
            (field,) = far(*args, both, field)
            if move == n - 2:
                cur_in, below, above = lax.optimization_barrier((cur, below, above))
                near_part = near(near_tgt[0], near_src[0], below_rim, cur_in, above_rim, near_blocks)
                top = top_up(me1, packs, coupling_share.shape[0])
                tops = lax.all_gather(top, "leaf", axis=0)
                mid_field = top_down(me1, top_list[0], packs, tops)
        else:
            to_below, to_above = far(*args, (0, 2), field, 2)
            from_above = shifted(to_below, "leaf", -1)
            from_below = shifted(to_above, "leaf", 1)
            (own,) = far(*args, (1,), field)

    out = down(
        leaf_rank, own, from_below, from_above, near_part, leaf_transfer, leaf_basis, mid_field
    )
    return out.reshape(leaves * panel, cols)


def solution(mesh):
    placed = (
        P(("leaf", "sub"), None),
        P(("leaf", "sub"), None, None),
        P(("leaf", "sub")),
        P(("leaf", "sub"), None, None),
        P("leaf", None, None, "sub"),
        P(),
        P(("leaf", "sub"), None, None, None),
        P(("leaf", "sub"), None, None, None),
        P(("leaf", "sub"), None, None, None),
        P("leaf", None, None, "sub", None),
        P("leaf", None),
        P(("leaf", "sub"), None, None, None),
        P(("leaf", "sub"), None),
        P(("leaf", "sub"), None),
    )
    return jax.shard_map(
        per_device, mesh=mesh, in_specs=placed, out_specs=P(("leaf", "sub"), None), check_vma=False
    )
```
